8 devices in a mesh: dp: 1 (over z), tp: 2 (over y), cp: 4 (over x, core).
Axes of the slice: x: 2, y: 2, z: 1, core: 2. Of those that a mesh axis runs over, the one named last changes fastest.
Arguments:
- hidden: bfloat16 [4096, 2560], P(('dp', 'cp'))
- start_pos: int32 [1], P('dp')
- k_local: bfloat16 [1024, 4, 256], P('dp', 'tp')
- v_local: bfloat16 [1024, 4, 256], P('dp', 'tp')
- k_global: bfloat16 [24576, 4, 256], P(('dp', 'cp'), 'tp')
- v_global: bfloat16 [24576, 4, 256], P(('dp', 'cp'), 'tp')
- w_query: bfloat16 [2, 2560, 2048], P(None, None, 'tp')
- w_key: bfloat16 [2, 2560, 1024], P(None, None, 'tp')
- w_value: bfloat16 [2, 2560, 1024], P(None, None, 'tp')
- w_out: bfloat16 [2, 2048, 2560], P(None, 'tp')
- w_gate: bfloat16 [2, 2560, 10240], P(None, None, 'tp')
- w_up: bfloat16 [2, 2560, 10240], P(None, None, 'tp')
- w_down: bfloat16 [2, 10240, 2560], P(None, 'tp')
- norm_gain: float32 [2, 4, 2560], replicated
- qk_gain: float32 [2, 2, 256], replicated
Outputs:
- output 1: bfloat16 [4096, 2560], P(('dp', 'cp'))
- output 2: bfloat16 [4096, 4, 256], P(('dp', 'cp'), 'tp')
- output 3: bfloat16 [4096, 4, 256], P(('dp', 'cp'), 'tp')
- output 4: bfloat16 [4096, 4, 256], P(('dp', 'cp'), 'tp')
- output 5: bfloat16 [4096, 4, 256], P(('dp', 'cp'), 'tp')
All inputs are finite; a program needn't handle non-finite values.
Results may differ from the reference program's by a relative error of at most 0.0198273.
Values are sent between devices in bfloat16 or wider.
A program may use at most 1 GiB of HBM per device.

```python
import jax
import jax.numpy as jnp
from jax import lax

MODEL_DIM = 2560
NUM_HEADS = 8
KV_HEADS = 4
HEAD_DIM = 256
FFN_DIM = 10240
WINDOW = 1024
CHUNK_LEN = 4096
CACHE_LEN = 24576
CACHE_SHARD = 6144
QUERY_BLOCK = 32

GROUPS = NUM_HEADS // KV_HEADS
NORM_EPS = 1e-6
LOCAL_BASE = 10000.0
GLOBAL_BASE = 1000000.0
GLOBAL_DIV = 8.0


def setup_inputs(seed: int = 0, part: int = 0) -> dict:
    part_key = jax.random.fold_in(jax.random.key(seed), part)
    own_keys = jax.random.split(part_key, 6)
    shared_keys = jax.random.split(jax.random.key(seed + 1), 9)

    def weight(draw_key, arr_shape, fan_in):
        return (jax.random.normal(draw_key, arr_shape, jnp.float32) * fan_in ** -0.5).astype(jnp.bfloat16)

    def unit_draw(draw_key, arr_shape):
        return jax.random.normal(draw_key, arr_shape, jnp.float32).astype(jnp.bfloat16)

    q_cols = NUM_HEADS * HEAD_DIM
    kv_cols = KV_HEADS * HEAD_DIM
    offset = jax.random.randint(own_keys[1], (1,), 0, CACHE_SHARD // 2 + 1)
    return {
        'hidden': unit_draw(own_keys[0], (CHUNK_LEN, MODEL_DIM)),
        'start_pos': (CACHE_LEN - offset).astype(jnp.int32),
        'k_local': unit_draw(own_keys[2], (WINDOW, KV_HEADS, HEAD_DIM)),
        'v_local': unit_draw(own_keys[3], (WINDOW, KV_HEADS, HEAD_DIM)),
        'k_global': unit_draw(own_keys[4], (CACHE_LEN, KV_HEADS, HEAD_DIM)),
        'v_global': unit_draw(own_keys[5], (CACHE_LEN, KV_HEADS, HEAD_DIM)),
        'w_query': weight(shared_keys[0], (2, MODEL_DIM, q_cols), MODEL_DIM),
        'w_key': weight(shared_keys[1], (2, MODEL_DIM, kv_cols), MODEL_DIM),
        'w_value': weight(shared_keys[2], (2, MODEL_DIM, kv_cols), MODEL_DIM),
        'w_out': weight(shared_keys[3], (2, q_cols, MODEL_DIM), q_cols),
        'w_gate': weight(shared_keys[4], (2, MODEL_DIM, FFN_DIM), MODEL_DIM),
        'w_up': weight(shared_keys[5], (2, MODEL_DIM, FFN_DIM), MODEL_DIM),
        'w_down': weight(shared_keys[6], (2, FFN_DIM, MODEL_DIM), FFN_DIM),
        'norm_gain': 0.3 * jax.random.normal(shared_keys[7], (2, 4, MODEL_DIM), jnp.float32),
        'qk_gain': 0.3 * jax.random.normal(shared_keys[8], (2, 2, HEAD_DIM), jnp.float32),
    }


def rms_scale(values, gain_vec):
    return values * lax.rsqrt(jnp.mean(values * values, axis=-1, keepdims=True) + NORM_EPS) * (1.0 + gain_vec)


def rotate(values, positions, rope_base, divisor):
    half_dim = values.shape[-1] // 2
    inv_freq = 1.0 / (rope_base ** (jnp.arange(0, 2 * half_dim, 2, dtype=jnp.float32) / (2 * half_dim)))
    angles = (positions.astype(jnp.float32) / divisor)[:, None] * inv_freq[None, :]
    angles = jnp.concatenate([angles, angles], axis=-1)[:, None, :]
    turned = jnp.concatenate([-values[..., half_dim:], values[..., :half_dim]], axis=-1)
    return values * jnp.cos(angles) + turned * jnp.sin(angles)


def attention(queries, key_all, value_all, query_pos, key_pos, key_ok, window):
    block_count = CHUNK_LEN // QUERY_BLOCK
    head_queries = jnp.transpose(queries.reshape(block_count, QUERY_BLOCK, KV_HEADS, GROUPS, HEAD_DIM), (2, 0, 1, 3, 4))
    pos_blocks = query_pos.reshape(block_count, QUERY_BLOCK)

    def per_head(head_args):
        block_queries, head_keys, head_values = head_args
        keys_f = head_keys.astype(jnp.float32)
        values_f = head_values.astype(jnp.float32)

        def per_block(block_args):
            one_block, block_pos = block_args
            scores = jnp.einsum('qgd,td->qgt', one_block.astype(jnp.float32), keys_f) * HEAD_DIM ** -0.5
            distance = block_pos[:, None] - key_pos[None, :]
            visible = key_ok[None, :] & (distance >= 0) & (distance < window)
            scores = jnp.where(visible[:, None, :], scores, -1e30)
            attn_prob = jax.nn.softmax(scores, axis=-1).astype(jnp.bfloat16)
            return jnp.einsum('qgt,td->qgd', attn_prob.astype(jnp.float32), values_f).astype(jnp.bfloat16)

        return lax.map(per_block, (block_queries, pos_blocks))

    head_out = lax.map(per_head, (head_queries, jnp.transpose(key_all, (1, 0, 2)), jnp.transpose(value_all, (1, 0, 2))))
    return jnp.transpose(head_out, (1, 2, 0, 3, 4)).reshape(CHUNK_LEN, NUM_HEADS * HEAD_DIM)


def decoder_layer(hidden, positions, layer_gains, qk_pair, w_query, w_key, w_value, w_out, w_gate, w_up, w_down, past_k, past_v, past_pos, past_ok, rope_base, divisor, window):
    normed = rms_scale(hidden.astype(jnp.float32), layer_gains[0]).astype(jnp.bfloat16)
    queries = jnp.dot(normed, w_query, preferred_element_type=jnp.float32).reshape(CHUNK_LEN, NUM_HEADS, HEAD_DIM)
    key_new = jnp.dot(normed, w_key, preferred_element_type=jnp.float32).reshape(CHUNK_LEN, KV_HEADS, HEAD_DIM)
    value_new = jnp.dot(normed, w_value, preferred_element_type=jnp.float32).astype(jnp.bfloat16).reshape(CHUNK_LEN, KV_HEADS, HEAD_DIM)
    queries = rotate(rms_scale(queries, qk_pair[0]), positions, rope_base, divisor).astype(jnp.bfloat16)
    key_new = rotate(rms_scale(key_new, qk_pair[1]), positions, rope_base, divisor).astype(jnp.bfloat16)
    key_all = jnp.concatenate([past_k, key_new], axis=0)
    value_all = jnp.concatenate([past_v, value_new], axis=0)
    key_pos = jnp.concatenate([past_pos, positions])
    key_ok = jnp.concatenate([past_ok, jnp.ones((CHUNK_LEN,), dtype=bool)])
    attn_out = attention(queries, key_all, value_all, positions, key_pos, key_ok, window)
    attn_proj = jnp.dot(attn_out, w_out, preferred_element_type=jnp.float32).astype(jnp.bfloat16)
    residual = (hidden.astype(jnp.float32) + rms_scale(attn_proj.astype(jnp.float32), layer_gains[1])).astype(jnp.bfloat16)
    normed = rms_scale(residual.astype(jnp.float32), layer_gains[2]).astype(jnp.bfloat16)
    gate_proj = jnp.dot(normed, w_gate, preferred_element_type=jnp.float32)
    up_proj = jnp.dot(normed, w_up, preferred_element_type=jnp.float32)
    hidden_act = (jax.nn.gelu(gate_proj, approximate=True) * up_proj).astype(jnp.bfloat16)
    down_proj = jnp.dot(hidden_act, w_down, preferred_element_type=jnp.float32).astype(jnp.bfloat16)
    layer_out = (residual.astype(jnp.float32) + rms_scale(down_proj.astype(jnp.float32), layer_gains[3])).astype(jnp.bfloat16)
    return layer_out, key_new, value_new


def reference(hidden, start_pos, k_local, v_local, k_global, v_global, w_query, w_key, w_value, w_out, w_gate, w_up, w_down, norm_gain, qk_gain):
    first_pos = start_pos[0]
    positions = first_pos + jnp.arange(CHUNK_LEN)
    slot_pos = first_pos - WINDOW + jnp.remainder(jnp.arange(WINDOW) - first_pos, WINDOW)
    middle, key_loc, value_loc = decoder_layer(hidden, positions, norm_gain[0], qk_gain[0], w_query[0], w_key[0], w_value[0], w_out[0], w_gate[0], w_up[0], w_down[0], k_local, v_local, slot_pos, jnp.ones((WINDOW,), dtype=bool), LOCAL_BASE, 1.0, WINDOW)
    cache_index = jnp.arange(CACHE_LEN)
    final_out, key_glob, value_glob = decoder_layer(middle, positions, norm_gain[1], qk_gain[1], w_query[1], w_key[1], w_value[1], w_out[1], w_gate[1], w_up[1], w_down[1], k_global, v_global, cache_index, cache_index < first_pos, GLOBAL_BASE, GLOBAL_DIV, CACHE_LEN + CHUNK_LEN + 1)
    return (final_out, key_loc, value_loc, key_glob, value_glob)
```

```python
import functools

import jax
import jax.numpy as jnp
from jax import lax
from jax.experimental import pallas as pl
from jax.experimental.pallas import tpu as pltpu
from jax.sharding import PartitionSpec as P

F32 = jnp.float32
BF16 = jnp.bfloat16
EPS = 1e-6
NEG = -1e30
LOG2E = 1.4426950408889634
HD = 256
VMEM_MAX = 63 * 2**20
ROW = ('arbitrary',)


def cost(flops, nbytes, trans=0):
    return pl.CostEstimate(flops=int(flops), bytes_accessed=int(nbytes), transcendentals=int(trans))


def params(n_axes):
    return pltpu.CompilerParams(dimension_semantics=('arbitrary',) * n_axes, vmem_limit_bytes=VMEM_MAX)


def rms(t, gain):
    return t * lax.rsqrt(jnp.mean(t * t, axis=-1, keepdims=True) + EPS) * (1.0 + gain)


def qkv_kernel(combine, n_q, n_kv, *refs):
    if combine:
        (x_ref, d0_ref, d1_ref, gd_ref, g_ref, qk_ref, wq_ref, wk_ref, wv_ref, cos_ref, sin_ref), rest = refs[:11], refs[11:]
    else:
        (x_ref, g_ref, qk_ref, wq_ref, wk_ref, wv_ref, cos_ref, sin_ref), rest = refs[:8], refs[8:]
    n_out = 4 if combine else 3
    outs = rest[len(rest) - n_out:]
    q_ref, k_ref, v_ref = outs[:3]
    x = x_ref[...].astype(F32)
    if combine:
        d = (d0_ref[...].astype(F32) + d1_ref[...].astype(F32)).astype(BF16).astype(F32)
        mid = (x + rms(d, gd_ref[...])).astype(BF16)
        outs[3][...] = mid
        x = mid.astype(F32)
    h = rms(x, g_ref[...]).astype(BF16)
    cos, sin = cos_ref[...], sin_ref[...]

    def turn(t, gain):
        t = rms(t, gain)
        lo, hi = t[:, :HD // 2], t[:, HD // 2:]
        return jnp.concatenate([lo * cos - hi * sin, hi * cos + lo * sin], axis=1).astype(BF16)

    kf = jnp.dot(h, wk_ref[0], preferred_element_type=F32)
    for n in range(n_kv):
        k_ref[:, n * HD:(n + 1) * HD] = turn(kf[:, n * HD:(n + 1) * HD], qk_ref[1:2, :])
    v_ref[...] = jnp.dot(h, wv_ref[0], preferred_element_type=F32).astype(BF16)
    qf = jnp.dot(h, wq_ref[0], preferred_element_type=F32)
    for n in range(n_q):
        q_ref[n] = turn(qf[:, n * HD:(n + 1) * HD], qk_ref[0:1, :])


def qkv(layer, x, d_pair, gd, gain, qk, wq, wk, wv, cos, sin, total_rows, row0, carried, tile=256):
    rows, dim = x.shape
    n_q, n_kv = wq.shape[2] // HD, wk.shape[2] // HD
    combine = d_pair is not None
    t0 = row0 // tile
    rowb = pl.BlockSpec((tile, dim), lambda i: (i, 0))
    vec = pl.BlockSpec((1, dim), lambda i: (0, 0))
    wspec = lambda w: pl.BlockSpec((1, dim, w.shape[2]), lambda i: (layer, 0, 0))
    trig = pl.BlockSpec((tile, HD // 2), lambda i: (i + t0, 0))
    ins, specs = [x], [rowb]
    if combine:
        ins += [d_pair[0], d_pair[1], gd]
        specs += [rowb, rowb, vec]
    ins += [gain, qk, wq, wk, wv, cos, sin]
    specs += [vec, pl.BlockSpec((2, HD), lambda i: (0, 0)), wspec(wq), wspec(wk), wspec(wv), trig, trig]
    aliases = {}
    if carried is not None:
        for j, arr in enumerate(carried):
            aliases[len(ins)] = j
            ins.append(arr)
            specs.append(pl.BlockSpec(memory_space=pl.ANY))
    out_shape = [jax.ShapeDtypeStruct((n_q, total_rows, HD), BF16), jax.ShapeDtypeStruct((total_rows, n_kv * HD), BF16), jax.ShapeDtypeStruct((total_rows, n_kv * HD), BF16)]
    out_specs = [pl.BlockSpec((n_q, tile, HD), lambda i: (0, i + t0, 0)), pl.BlockSpec((tile, n_kv * HD), lambda i: (i + t0, 0)), pl.BlockSpec((tile, n_kv * HD), lambda i: (i + t0, 0))]
    if combine:
        out_shape.append(jax.ShapeDtypeStruct((rows, dim), BF16))
        out_specs.append(rowb)
    cols = (n_q + 2 * n_kv) * HD
    return pl.pallas_call(
        functools.partial(qkv_kernel, combine, n_q, n_kv),
        grid=(rows // tile,), in_specs=specs, out_specs=out_specs, out_shape=out_shape,
        input_output_aliases=aliases, compiler_params=params(1),
        cost_estimate=cost(2 * rows * dim * cols, 2 * (rows * dim + dim * cols + rows * cols)), name='qkv')(*ins)


def window_kernel(tile, tiles, win, q_ref, kp_ref, vp_ref, ko_ref, vo_ref, o_ref):
    scale = LOG2E * HD ** -0.5
    rows2 = 2 * tile
    row = lax.broadcasted_iota(jnp.int32, (rows2, tile), 0) & (tile - 1)
    col = lax.broadcasted_iota(jnp.int32, (rows2, tile), 1)
    nb = win // tile
    for j, t in enumerate(tiles):
        q = q_ref[:, t * tile:(t + 1) * tile, :].reshape(rows2, HD)
        pieces = []
        for b in range(t, t + nb + 1):
            pieces.append((kp_ref, vp_ref, b * tile) if b < nb else (ko_ref, vo_ref, (b - nb) * tile))
        ss = []
        for i, (kr, _, st) in enumerate(pieces):
            s = lax.dot_general(q, kr[st:st + tile, :], (((1,), (1,)), ((), ())), preferred_element_type=F32) * scale
            if i == 0:
                s = jnp.where(col > row, s, NEG)
            if i == nb:
                s = jnp.where(col <= row, s, NEG)
            ss.append(s)
        top = ss[0]
        for s in ss[1:]:
            top = jnp.maximum(top, s)
        top = top.max(axis=1, keepdims=True)
        total = jnp.zeros((rows2, tile), F32)
        acc = jnp.zeros((rows2, HD), F32)
        for s, (_, vr, st) in zip(ss, pieces):
            p = jnp.exp2(s - top)
            total = total + p
            acc = acc + jnp.dot(p.astype(BF16), vr[st:st + tile, :], preferred_element_type=F32)
        out = (acc / total.sum(axis=1, keepdims=True)).astype(BF16)
        for g in range(2):
            o_ref[j * tile:(j + 1) * tile, g * HD:(g + 1) * HD] = out[g * tile:(g + 1) * tile]


def window_attention(q, kp, vp, ko, vo, row0, rows, tile=256):
    n_q = q.shape[0]
    n_kv = n_q // 2
    win = kp.shape[0]
    total = q.shape[1]
    tiles = tuple(range(row0 // tile, (row0 + rows) // tile))
    kv = lambda n: pl.BlockSpec((n, HD), lambda h: (0, h))
    return pl.pallas_call(
        functools.partial(window_kernel, tile, tiles, win),
        grid=(n_kv,),
        in_specs=[pl.BlockSpec((2, total, HD), lambda h: (h, 0, 0)), kv(win), kv(win), kv(total), kv(total)],
        out_specs=pl.BlockSpec((rows, 2 * HD), lambda h: (0, h)),
        out_shape=jax.ShapeDtypeStruct((rows, n_q * HD), BF16),
        compiler_params=params(1),
        cost_estimate=cost(4 * rows * n_q * (win + tile) * HD, 2 * (4 * total * n_kv * HD + 2 * rows * n_q * HD)), name='window')(q, kp, vp, ko, vo)


def split3(x):
    hi = x.astype(BF16)
    r = x - hi.astype(F32)
    mid = r.astype(BF16)
    return hi, mid, (r - mid.astype(F32)).astype(BF16)


def global_kernel(bq, bk, ns, sc_ref, q_ref, kc_ref, vc_ref, kn_ref, vn_ref, o_ref, aux_ref, m_ref, l_ref, acc_ref):
    head = pl.program_id(0)
    qt = pl.program_id(1)
    n_valid = sc_ref[0]
    delta = sc_ref[1]
    scale = LOG2E * HD ** -0.5
    m_ref[...] = jnp.full_like(m_ref, NEG)
    l_ref[...] = jnp.zeros_like(l_ref)
    acc_ref[...] = jnp.zeros_like(acc_ref)
    rs = 2 * bq // ns

    def block(k_ref, v_ref, start, mask_fn):
        k = k_ref[pl.ds(start, bk), :]
        v = v_ref[pl.ds(start, bk), :]
        ss = []
        for c in range(ns):
            g, r0 = divmod(c * rs, bq)
            s = lax.dot_general(q_ref[g, r0:r0 + rs, :], k, (((1,), (1,)), ((), ())), preferred_element_type=F32) * scale
            if mask_fn is not None:
                s = jnp.where(mask_fn(r0, rs), s, NEG)
            ss.append(s)
        for c, s in enumerate(ss):
            rows = slice(c * rs, (c + 1) * rs)
            m_prev = m_ref[rows, :]
            m_new = jnp.maximum(m_prev, s.max(axis=1, keepdims=True))
            alpha = jnp.exp2(m_prev - m_new)
            l = l_ref[rows, :] * alpha
            ps = []
            for j in range(bk // 128):
                p = jnp.exp2(s[:, j * 128:(j + 1) * 128] - m_new)
                l = l + p
                ps.append(p.astype(BF16))
            l_ref[rows, :] = l
            m_ref[rows, :] = m_new
            pv = jnp.dot(jnp.concatenate(ps, axis=1), v, preferred_element_type=F32)
            for j in range(HD // 128):
                cs = slice(j * 128, (j + 1) * 128)
                acc_ref[rows, cs] = acc_ref[rows, cs] * alpha + pv[:, cs]

    n_full = n_valid // bk

    def cache_step(i, c):
        block(kc_ref, vc_ref, pl.multiple_of(i * bk, bk), None)
        return c

    lax.fori_loop(0, n_full, cache_step, 0)

    @pl.when(n_full * bk < n_valid)
    def _():
        start = pl.multiple_of(n_full * bk, bk)
        block(kc_ref, vc_ref, start, lambda r0, n: (start + lax.broadcasted_iota(jnp.int32, (n, bk), 1)) < n_valid)

    n_new = kn_ref.shape[0]
    row0 = qt * bq + delta
    own_full = jnp.clip((row0 + 1) // bk, 0, n_new // bk)
    own_any = jnp.clip((row0 + bq + bk - 1) // bk, 0, n_new // bk)

    def own_step(i, c):
        block(kn_ref, vn_ref, pl.multiple_of(i * bk, bk), None)
        return c

    lax.fori_loop(0, own_full, own_step, 0)

    def diag_step(i, c):
        start = pl.multiple_of(i * bk, bk)

        def mask(r0, n):
            key = start + lax.broadcasted_iota(jnp.int32, (n, bk), 1)
            return key <= row0 + r0 + lax.broadcasted_iota(jnp.int32, (n, bk), 0)

        block(kn_ref, vn_ref, start, mask)
        return c

    lax.fori_loop(own_full, own_any, diag_step, 0)
    lane = lax.broadcasted_iota(jnp.int32, (bq, 128), 1)
    row_sl = pl.ds(pl.multiple_of(qt * bq, bq), bq)
    aux = aux_ref[row_sl, :]
    for g in range(2):
        rows = slice(g * bq, (g + 1) * bq)
        l = l_ref[rows, :].sum(axis=1, keepdims=True)
        o_ref[:, g * HD:(g + 1) * HD] = (acc_ref[rows, :] / l).astype(BF16)
        lse = m_ref[rows, :] + jnp.log2(l)
        for p, part in enumerate(split3(lse)):
            aux = jnp.where(lane == 16 * (2 * head + g) + p, part, aux)
    aux_ref[row_sl, :] = aux


def global_attention(q, kc, vc, kn, vn, sc, bk=1024, ns=4):
    n_q, rows, _ = q.shape
    bq = min(rows, 1024)
    n_kv = n_q // 2
    kv = lambda a: pl.BlockSpec((a.shape[0], HD), lambda h, t, *_: (0, h))
    keys = kc.shape[0] + kn.shape[0]
    return pl.pallas_call(
        functools.partial(global_kernel, bq, bk, ns),
        grid_spec=pltpu.PrefetchScalarGridSpec(
            num_scalar_prefetch=1, grid=(n_kv, rows // bq),
            in_specs=[pl.BlockSpec((2, bq, HD), lambda h, t, *_: (h, t, 0)), kv(kc), kv(vc), kv(kn), kv(vn)],
            out_specs=[pl.BlockSpec((bq, 2 * HD), lambda h, t, *_: (t, h)), pl.BlockSpec((rows, 128), lambda h, t, *_: (0, 0))],
            scratch_shapes=[pltpu.VMEM((2 * bq, 128), F32), pltpu.VMEM((2 * bq, 128), F32), pltpu.VMEM((2 * bq, HD), F32)]),
        out_shape=[jax.ShapeDtypeStruct((rows, n_q * HD), BF16), jax.ShapeDtypeStruct((rows, 128), BF16)],
        compiler_params=params(2),
        cost_estimate=cost(4 * rows * n_q * keys * HD, 2 * (2 * keys * n_kv * HD + 2 * rows * n_q * HD), rows * n_q * keys),
        name='gattn')(sc, q, kc, vc, kn, vn)


def merge_kernel(n, n_q, *refs):
    parts, auxs = refs[:n], refs[n:2 * n]
    o_ref = refs[2 * n]
    aux_out = refs[2 * n + 1] if len(refs) > 2 * n + 1 else None
    rows = o_ref.shape[0]
    lane = lax.broadcasted_iota(jnp.int32, (rows, 128), 1)
    new_aux = jnp.zeros((rows, 128), BF16)
    for h in range(n_q):
        lses = []
        for a in auxs:
            c = a[:, 16 * h:16 * h + 3].astype(F32)
            lses.append(c[:, 0:1] + c[:, 1:2] + c[:, 2:3])
        top = functools.reduce(jnp.maximum, lses)
        ws = [jnp.exp2(s - top) for s in lses]
        total = functools.reduce(jnp.add, ws)
        cs = slice(h * HD, (h + 1) * HD)
        o = functools.reduce(jnp.add, [p[:, cs].astype(F32) * (w / total) for p, w in zip(parts, ws)])
        o_ref[:, cs] = o.astype(BF16)
        if aux_out is not None:
            lse = jnp.broadcast_to(top + jnp.log2(total), (rows, 128))
            for p, part in enumerate(split3(lse)):
                new_aux = jnp.where(lane == 16 * h + p, part, new_aux)
    if aux_out is not None:
        aux_out[...] = new_aux


def merge(parts, row0, rows, keep_aux, tile=256):
    n = len(parts)
    width = parts[0][0].shape[1]
    t0 = row0 // tile
    big = lambda i: (i + t0, 0)
    out_shape = [jax.ShapeDtypeStruct((rows, width), BF16)]
    out_specs = [pl.BlockSpec((tile, width), lambda i: (i, 0))]
    if keep_aux:
        out_shape.append(jax.ShapeDtypeStruct((rows, 128), BF16))
        out_specs.append(pl.BlockSpec((tile, 128), lambda i: (i, 0)))
    return pl.pallas_call(
        functools.partial(merge_kernel, n, width // HD), grid=(rows // tile,),
        in_specs=[pl.BlockSpec((tile, width), big)] * n + [pl.BlockSpec((tile, 128), big)] * n,
        out_specs=out_specs, out_shape=out_shape, compiler_params=params(1),
        cost_estimate=cost(8e6, 2 * (n + 1) * rows * width), name='merge')(*[p[0] for p in parts], *[p[1] for p in parts])


def wo_kernel(tp_ref, x_ref, o0_ref, o1_ref, w_ref, ga_ref, gu_ref, x1_ref, u_ref):
    own, other = o0_ref[...], o1_ref[...]
    first = tp_ref[0] == 0
    o = jnp.concatenate([jnp.where(first, own, other), jnp.where(first, other, own)], axis=1)
    a = jnp.dot(o, w_ref[...], preferred_element_type=F32).astype(BF16).astype(F32)
    x1 = (x_ref[...].astype(F32) + rms(a, ga_ref[...])).astype(BF16)
    x1_ref[...] = x1
    u_ref[...] = rms(x1.astype(F32), gu_ref[...]).astype(BF16)


def out_proj(tp, x, o_own, o_other, w, ga, gu, row0, tile=256):
    rows, half = o_own.shape
    dim = w.shape[1]
    t0 = row0 // tile
    rowb = pl.BlockSpec((tile, dim), lambda i, *_: (i, 0))
    vec = pl.BlockSpec((1, dim), lambda i, *_: (0, 0))
    ob = pl.BlockSpec((tile, half), lambda i, *_: (i, 0))
    return pl.pallas_call(
        wo_kernel,
        grid_spec=pltpu.PrefetchScalarGridSpec(
            num_scalar_prefetch=1, grid=(rows // tile,),
            in_specs=[pl.BlockSpec((tile, dim), lambda i, *_: (i + t0, 0)), ob, ob, pl.BlockSpec(w.shape, lambda i, *_: (0, 0)), vec, vec],
            out_specs=[rowb, rowb]),
        out_shape=[jax.ShapeDtypeStruct((rows, dim), BF16)] * 2, compiler_params=params(1),
        cost_estimate=cost(4 * rows * half * dim, 2 * (2 * half * dim + 3 * rows * dim)), name='wo')(tp, x, o_own, o_other, w, ga, gu)


def ffn_kernel(nb, u_ref, wg_ref, wu_ref, wd_ref, d_ref, act_ref, acc_ref):
    n = pl.program_id(0)

    def head(slot):
        g = jnp.dot(u_ref[...], wg_ref[0], preferred_element_type=F32)
        up = jnp.dot(u_ref[...], wu_ref[0], preferred_element_type=F32)
        act_ref[slot] = (jax.nn.gelu(g, approximate=True) * up).astype(BF16)

    def tail(slot):
        return jnp.dot(act_ref[slot], wd_ref[0], preferred_element_type=F32)

    @pl.when(n == 0)
    def _():
        head(0)
        acc_ref[...] = jnp.zeros_like(acc_ref)

    for slot in range(2):
        @pl.when((n > 0) & (n < nb) & (n % 2 == slot))
        def _():
            acc_ref[...] += tail(1 - slot)
            head(slot)

    @pl.when(n == nb)
    def _():
        d_ref[...] = (acc_ref[...] + tail((nb - 1) % 2)).astype(BF16)


def ffn(layer, u, wg, wu, wd, bn=512):
    rows, dim = u.shape
    width = wg.shape[2]
    nb = width // bn
    return pl.pallas_call(
        functools.partial(ffn_kernel, nb), grid=(nb + 1,),
        in_specs=[pl.BlockSpec((rows, dim), lambda n: (0, 0)),
                  pl.BlockSpec((1, dim, bn), lambda n: (layer, 0, jnp.minimum(n, nb - 1))),
                  pl.BlockSpec((1, dim, bn), lambda n: (layer, 0, jnp.minimum(n, nb - 1))),
                  pl.BlockSpec((1, bn, dim), lambda n: (layer, jnp.maximum(n - 1, 0), 0))],
        out_specs=pl.BlockSpec((rows, dim), lambda n: (0, 0)),
        out_shape=jax.ShapeDtypeStruct((rows, dim), BF16),
        scratch_shapes=[pltpu.VMEM((2, rows, bn), BF16), pltpu.VMEM((rows, dim), F32)],
        compiler_params=params(1),
        cost_estimate=cost(6 * rows * dim * width, 2 * (3 * dim * width + 2 * rows * dim), rows * width), name='ffn')(u, wg, wu, wd)


def last_kernel(x_ref, d0_ref, d1_ref, g_ref, *rest):
    d = (d0_ref[...].astype(F32) + d1_ref[...].astype(F32)).astype(BF16).astype(F32)
    rest[-1][...] = (x_ref[...].astype(F32) + rms(d, g_ref[...])).astype(BF16)


def last(x, d_pair, gain, total_rows, row0, carried, tile=256):
    rows, dim = x.shape
    t0 = row0 // tile
    rowb = pl.BlockSpec((tile, dim), lambda i: (i, 0))
    ins = [x, d_pair[0], d_pair[1], gain]
    specs = [rowb, rowb, rowb, pl.BlockSpec((1, dim), lambda i: (0, 0))]
    aliases = {}
    if carried is not None:
        aliases[4] = 0
        ins.append(carried)
        specs.append(pl.BlockSpec(memory_space=pl.ANY))
    return pl.pallas_call(
        last_kernel, grid=(rows // tile,), in_specs=specs,
        out_specs=pl.BlockSpec((tile, dim), lambda i: (i + t0, 0)),
        out_shape=jax.ShapeDtypeStruct((total_rows, dim), BF16), input_output_aliases=aliases,
        compiler_params=params(1), cost_estimate=cost(10 * rows * dim, 8 * rows * dim), name='last')(*ins)


def rope_tables(positions, base, divisor):
    inv_freq = 1.0 / (base ** (jnp.arange(0, HD, 2, dtype=F32) / HD))
    angles = (positions.astype(F32) / divisor)[:, None] * inv_freq[None, :]
    return jnp.cos(angles), jnp.sin(angles)


def solution(mesh):
    cp_size = mesh.shape['cp']
    tp_size = mesh.shape['tp']
    row_spec = P(('dp', 'cp'), None)
    cache_spec = P(('dp', 'cp'), 'tp', None)
    window_spec = P('dp', 'tp', None)
    col_spec = P(None, None, 'tp')
    row_split = P(None, 'tp', None)
    replicated = P()
    swap_tp = [(i, tp_size - 1 - i) for i in range(tp_size)]
    chunks = 2

    def xor(k):
        return [(i, i ^ k) for i in range(cp_size)]

    def device_step(hidden, start_pos, k_local, v_local, k_global, v_global, w_query, w_key, w_value, w_out, w_gate, w_up, w_down, norm_gain, qk_gain):
        first_pos = start_pos[0]
        cp_index = lax.axis_index('cp')
        tp_index = lax.axis_index('tp')
        tp = tp_index.astype(jnp.int32)[None]
        rows = hidden.shape[0]
        part = rows // chunks
        n_kv = k_local.shape[1]
        shard_len = k_global.shape[0]
        positions = first_pos + cp_index * rows + jnp.arange(rows)
        gains = lambda l, i: norm_gain[l, i][None, :]

        quarter = w_out.shape[1] // cp_size
        w_full = []
        for l in range(2):
            piece = lax.dynamic_slice(w_out, (l, cp_index * quarter, 0), (1, quarter, w_out.shape[2]))[0]
            w_full.append(lax.all_gather(piece, ('tp', 'cp'), axis=0, tiled=True))

        def finish(l, x_of, o_parts):
            xs, us, ds = [], [], []
            others = [lax.ppermute(o, 'tp', swap_tp) for o in o_parts]
            for i in range(chunks):
                x, r0 = x_of(i)
                x1, u = out_proj(tp, x, o_parts[i], others[i], w_full[l], gains(l, 1), gains(l, 2), r0)
                d = ffn(l, u, w_gate, w_up, w_down)
                xs.append(x1)
                ds.append((d, lax.ppermute(d, 'tp', swap_tp)))
            return xs, ds

        cos, sin = rope_tables(positions, 10000.0, 1.0)
        q, k_loc, v_loc = qkv(0, hidden, None, None, gains(0, 0), qk_gain[0], w_query, w_key, w_value, cos, sin, rows, 0, None)
        ahead = [(i, i + 1) for i in range(cp_size - 1)]
        shift = jnp.remainder(first_pos, k_local.shape[0])

        def before(cache, new):
            rolled = jnp.roll(cache.reshape(cache.shape[0], -1), -shift, axis=0)
            return jnp.where(cp_index == 0, rolled, lax.ppermute(new, 'cp', ahead))

        k_prev, v_prev = before(k_local, k_loc), before(v_local, v_loc)
        o_parts = [window_attention(q, k_prev, v_prev, k_loc, v_loc, i * part, part) for i in range(chunks)]
        xs, ds = finish(0, lambda i: (hidden, i * part), o_parts)

        cos, sin = rope_tables(positions, 1000000.0, 8.0)
        carried, mids = None, []
        for i in range(chunks):
            *carried, mid = qkv(1, xs[i], ds[i], gains(0, 3), gains(1, 0), qk_gain[1], w_query, w_key, w_value, cos, sin, rows, i * part, carried)
            mids.append(mid)
        q, k_glob, v_glob = carried
        kc = k_global.reshape(shard_len, -1)
        vc = v_global.reshape(shard_len, -1)
        n_valid = jnp.clip(first_pos - cp_index * shard_len, 0, shard_len)

        def attend(block_q, owner):
            sc = jnp.stack([n_valid, (owner - cp_index) * rows]).astype(jnp.int32)
            return global_attention(block_q, kc, vc, k_glob, v_glob, sc)

        def move(pair, k):
            return [lax.ppermute(a, 'cp', xor(k)) for a in pair]

        q2 = lax.ppermute(q, 'cp', xor(2))
        q1 = lax.ppermute(q, 'cp', xor(1))
        q3 = lax.ppermute(q2, 'cp', xor(1))
        own = attend(q, cp_index)
        far3 = attend(q3, cp_index ^ 3)
        far2 = attend(q2, cp_index ^ 2)
        near = attend(q1, cp_index ^ 1)
        far = move(merge([far2, move(far3, 1)], 0, rows, True), 2)
        near = move(near, 1)
        o_parts = [merge([own, near, far], i * part, part, False)[0] for i in range(chunks)]
        xs, ds = finish(1, lambda i: (mids[i], 0), o_parts)
        out = None
        for i in range(chunks):
            out = last(xs[i], ds[i], gains(1, 3), rows, i * part, out)
        heads = lambda a: a.reshape(rows, n_kv, HD)
        return out, heads(k_loc), heads(v_loc), heads(k_glob), heads(v_glob)

    return jax.shard_map(device_step, mesh=mesh, in_specs=(row_spec, P('dp'), window_spec, window_spec, cache_spec, cache_spec, col_spec, col_spec, col_spec, row_split, col_spec, col_spec, row_split, replicated, replicated), out_specs=(row_spec, cache_spec, cache_spec, cache_spec, cache_spec), check_vma=False)
```

```python
import functools

import jax
import jax.numpy as jnp
from jax import lax
from jax.experimental import pallas as pl
from jax.experimental.pallas import tpu as pltpu
from jax.sharding import PartitionSpec as P

F32 = jnp.float32
BF16 = jnp.bfloat16
EPS = 1e-6
NEG = -1e30
LOG2E = 1.4426950408889634
HD = 256
VMEM_MAX = 63 * 2**20
ROW = ('arbitrary',)


def cost(flops, nbytes, trans=0):
    return pl.CostEstimate(flops=int(flops), bytes_accessed=int(nbytes), transcendentals=int(trans))


def params(n_axes):
    return pltpu.CompilerParams(dimension_semantics=('arbitrary',) * n_axes, vmem_limit_bytes=VMEM_MAX)


def rms(t, gain):
    return t * lax.rsqrt(jnp.mean(t * t, axis=-1, keepdims=True) + EPS) * (1.0 + gain)


def turn(t, gain, cos, sin):
    t = rms(t, gain)
    lo, hi = t[:, :HD // 2], t[:, HD // 2:]
    return jnp.concatenate([lo * cos - hi * sin, hi * cos + lo * sin], axis=1).astype(BF16)


def qkv_kernel(n_q, n_kv, x_ref, d0_ref, d1_ref, gd_ref, g_ref, qk_ref, wq_ref, wk_ref, wv_ref, cos_ref, sin_ref, q_ref, k_ref, v_ref, mid_ref):
    d = (d0_ref[...].astype(F32) + d1_ref[...].astype(F32)).astype(BF16).astype(F32)
    mid = (x_ref[...].astype(F32) + rms(d, gd_ref[...])).astype(BF16)
    mid_ref[...] = mid
    h = rms(mid.astype(F32), g_ref[...]).astype(BF16)
    cos, sin = cos_ref[...], sin_ref[...]
    kf = jnp.dot(h, wk_ref[0], preferred_element_type=F32)
    for n in range(n_kv):
        k_ref[:, n * HD:(n + 1) * HD] = turn(kf[:, n * HD:(n + 1) * HD], qk_ref[1:2, :], cos, sin)
    v_ref[...] = jnp.dot(h, wv_ref[0], preferred_element_type=F32).astype(BF16)
    qf = jnp.dot(h, wq_ref[0], preferred_element_type=F32)
    for n in range(n_q):
        q_ref[n] = turn(qf[:, n * HD:(n + 1) * HD], qk_ref[0:1, :], cos, sin)


def qkv(layer, x, d_pair, gd, gain, qk, wq, wk, wv, cos, sin, row0, tile=256):
    rows, dim = x.shape
    n_q, n_kv = wq.shape[2] // HD, wk.shape[2] // HD
    t0 = row0 // tile
    rowb = pl.BlockSpec((tile, dim), lambda i: (i, 0))
    vec = pl.BlockSpec((1, dim), lambda i: (0, 0))
    wspec = lambda w: pl.BlockSpec((1, dim, w.shape[2]), lambda i: (layer, 0, 0))
    trig = pl.BlockSpec((tile, HD // 2), lambda i: (i + t0, 0))
    kvb = pl.BlockSpec((tile, n_kv * HD), lambda i: (i, 0))
    cols = (n_q + 2 * n_kv) * HD
    return pl.pallas_call(
        functools.partial(qkv_kernel, n_q, n_kv), grid=(rows // tile,),
        in_specs=[rowb, rowb, rowb, vec, vec, pl.BlockSpec((2, HD), lambda i: (0, 0)), wspec(wq), wspec(wk), wspec(wv), trig, trig],
        out_specs=[pl.BlockSpec((n_q, tile, HD), lambda i: (0, i, 0)), kvb, kvb, rowb],
        out_shape=[jax.ShapeDtypeStruct((n_q, rows, HD), BF16)] + [jax.ShapeDtypeStruct((rows, n_kv * HD), BF16)] * 2 + [jax.ShapeDtypeStruct((rows, dim), BF16)],
        compiler_params=params(1),
        cost_estimate=cost(2 * rows * dim * cols, 2 * (rows * dim + dim * cols + rows * cols)), name='qkv')(x, *d_pair, gd, gain, qk, wq, wk, wv, cos, sin)


def kv_kernel(n_kv, steps, x_ref, g_ref, qk_ref, wk_ref, wv_ref, cos_ref, sin_ref, k0_ref, k1_ref, v0_ref, v1_ref, h_ref):
    i = pl.program_id(0)
    h = rms(x_ref[...].astype(F32), g_ref[...]).astype(BF16)
    h_ref[...] = h
    kf = jnp.dot(h, wk_ref[0], preferred_element_type=F32)
    k = jnp.concatenate([turn(kf[:, n * HD:(n + 1) * HD], qk_ref[1:2, :], cos_ref[...], sin_ref[...]) for n in range(n_kv)], axis=1)
    v = jnp.dot(h, wv_ref[0], preferred_element_type=F32).astype(BF16)

    @pl.when(i < steps // 2)
    def _():
        k0_ref[...] = k
        v0_ref[...] = v

    @pl.when(i >= steps // 2)
    def _():
        k1_ref[...] = k
        v1_ref[...] = v


def kv_first(layer, x, gain, qk, wk, wv, cos, sin, tile=256):
    rows, dim = x.shape
    cols = wk.shape[2]
    steps = rows // tile
    rowb = pl.BlockSpec((tile, dim), lambda i: (i, 0))
    wspec = pl.BlockSpec((1, dim, cols), lambda i: (layer, 0, 0))
    trig = pl.BlockSpec((tile, HD // 2), lambda i: (i, 0))
    lower = pl.BlockSpec((tile, cols), lambda i: (jnp.minimum(i, steps // 2 - 1), 0))
    upper = pl.BlockSpec((tile, cols), lambda i: (jnp.maximum(i - steps // 2, 0), 0))
    return pl.pallas_call(
        functools.partial(kv_kernel, cols // HD, steps), grid=(steps,),
        in_specs=[rowb, pl.BlockSpec((1, dim), lambda i: (0, 0)), pl.BlockSpec((2, HD), lambda i: (0, 0)), wspec, wspec, trig, trig],
        out_specs=[lower, upper, lower, upper, rowb],
        out_shape=[jax.ShapeDtypeStruct((rows // 2, cols), BF16)] * 4 + [jax.ShapeDtypeStruct((rows, dim), BF16)],
        compiler_params=params(1),
        cost_estimate=cost(4 * rows * dim * cols, 4 * (rows * dim + dim * cols + rows * cols)), name='kv')(x, gain, qk, wk, wv, cos, sin)


def q_kernel(n_q, h_ref, qk_ref, wq_ref, cos_ref, sin_ref, q_ref):
    qf = jnp.dot(h_ref[...], wq_ref[0], preferred_element_type=F32)
    for n in range(n_q):
        q_ref[n] = turn(qf[:, n * HD:(n + 1) * HD], qk_ref[0:1, :], cos_ref[...], sin_ref[...])


def q_after(layer, h, qk, wq, cos, sin, tile=512):
    rows, dim = h.shape
    n_q = wq.shape[2] // HD
    trig = pl.BlockSpec((tile, HD // 2), lambda i: (i, 0))
    return pl.pallas_call(
        functools.partial(q_kernel, n_q), grid=(rows // tile,),
        in_specs=[pl.BlockSpec((tile, dim), lambda i: (i, 0)), pl.BlockSpec((2, HD), lambda i: (0, 0)), pl.BlockSpec((1, dim, n_q * HD), lambda i: (layer, 0, 0)), trig, trig],
        out_specs=pl.BlockSpec((n_q, tile, HD), lambda i: (0, i, 0)),
        out_shape=jax.ShapeDtypeStruct((n_q, rows, HD), BF16), compiler_params=params(1),
        cost_estimate=cost(2 * rows * dim * n_q * HD, 2 * (rows + n_q * HD) * dim), name='q')(h, qk, wq, cos, sin)


def window_kernel(tile, tiles, halves, flag_ref, q_ref, *refs):
    n = len(halves)
    gots, caches, owns = refs[:2 * n], refs[2 * n:4 * n], refs[4 * n:4 * n + 4]
    o_ref = refs[4 * n + 4]
    prevs = refs[4 * n + 5:]
    first = flag_ref[0] == 0
    for p, g, c in zip(prevs, gots, caches):
        p[...] = jnp.where(first, c[...], g[...])
    scale = LOG2E * HD ** -0.5
    rows2 = 2 * tile
    row = lax.broadcasted_iota(jnp.int32, (rows2, tile), 0) & (tile - 1)
    col = lax.broadcasted_iota(jnp.int32, (rows2, tile), 1)
    each = owns[0].shape[0]
    nb = 2 * each // tile
    for j, t in enumerate(tiles):
        q = q_ref[:, t * tile:(t + 1) * tile, :].reshape(rows2, HD)
        pieces = []
        for b in range(t, t + nb + 1):
            half, st = divmod(b % nb * tile, each)
            kr, vr = (prevs[halves.index(half)], prevs[n + halves.index(half)]) if b < nb else (owns[half], owns[2 + half])
            pieces.append((kr, vr, st))
        ss = []
        for i, (kr, _, st) in enumerate(pieces):
            s = lax.dot_general(q, kr[st:st + tile, :], (((1,), (1,)), ((), ())), preferred_element_type=F32) * scale
            if i == 0:
                s = jnp.where(col > row, s, NEG)
            if i == nb:
                s = jnp.where(col <= row, s, NEG)
            ss.append(s)
        top = ss[0]
        for s in ss[1:]:
            top = jnp.maximum(top, s)
        top = top.max(axis=1, keepdims=True)
        total = jnp.zeros((rows2, tile), F32)
        acc = jnp.zeros((rows2, HD), F32)
        for s, (_, vr, st) in zip(ss, pieces):
            p = jnp.exp2(s - top)
            total = total + p
            acc = acc + jnp.dot(p.astype(BF16), vr[st:st + tile, :], preferred_element_type=F32)
        out = (acc / total.sum(axis=1, keepdims=True)).astype(BF16)
        for g in range(2):
            o_ref[j * tile:(j + 1) * tile, g * HD:(g + 1) * HD] = out[g * tile:(g + 1) * tile]


def window_attention(flag, q, got, cache, own, halves, row0, rows, tile=256):
    n_q, total, _ = q.shape
    n_kv = n_q // 2
    part = own[0].shape[0]
    tiles = tuple(range(row0 // tile, (row0 + rows) // tile))
    kv = lambda i: pl.BlockSpec((part, HD), lambda h, *_: (i, h))
    ins = [got[i][j] for j in range(2) for i in halves] + [cache[j] for j in range(2) for _ in halves] + list(own)
    specs = [kv(0)] * (2 * len(halves)) + [kv(i) for _ in range(2) for i in halves] + [kv(0)] * 4
    return pl.pallas_call(
        functools.partial(window_kernel, tile, tiles, tuple(halves)),
        grid_spec=pltpu.PrefetchScalarGridSpec(
            num_scalar_prefetch=1, grid=(n_kv,),
            in_specs=[pl.BlockSpec((2, total, HD), lambda h, *_: (h, 0, 0))] + specs,
            out_specs=pl.BlockSpec((rows, 2 * HD), lambda h, *_: (0, h)),
            scratch_shapes=[pltpu.VMEM((part, HD), BF16)] * (2 * len(halves))),
        out_shape=jax.ShapeDtypeStruct((rows, n_q * HD), BF16), compiler_params=params(1),
        cost_estimate=cost(4 * rows * n_q * (2 * part + tile) * HD, 2 * (4 * total * n_kv * HD + 2 * rows * n_q * HD)), name='window')(flag, q, *ins)


def split3(x):
    hi = x.astype(BF16)
    r = x - hi.astype(F32)
    mid = r.astype(BF16)
    return hi, mid, (r - mid.astype(F32)).astype(BF16)


def global_kernel(offsets, own, n_parts, bq, bk, use_cache, use_new, want_aux, *refs):
    halves = len(offsets)
    sc_ref, norm_ref, refs = refs[0], refs[1], refs[2:]
    qs, refs = refs[:halves], refs[halves:]
    if use_cache:
        (kc_ref, vc_ref), refs = refs[:2], refs[2:]
    if use_new:
        news, refs = refs[:4], refs[4:]
    parts, refs = refs[:2 * n_parts * halves], refs[2 * n_parts * halves:]
    per = 2 if want_aux else 1
    outs, refs = refs[:per * halves], refs[per * halves:]
    m_ref, l_ref, acc_ref = refs[:3]
    head = pl.program_id(0)
    scale = LOG2E * HD ** -0.5
    small = 256
    chains = [(hf, g) for hf in range(halves) for g in range(2)]
    rows_of = lambda hf, g: slice((2 * hf + g) * bq, (2 * hf + g + 1) * bq)
    l_ref[...] = jnp.zeros_like(l_ref)
    acc_ref[...] = jnp.zeros_like(acc_ref)
    if use_new:
        kn_ref, vn_ref = refs[3:5]
        half = news[0].shape[0]
        for i in range(2):
            kn_ref[i * half:(i + 1) * half, :] = news[i][...]
            vn_ref[i * half:(i + 1) * half, :] = news[2 + i][...]
    later = jnp.where(sc_ref[1] > 0, 1, 0) if use_new and not own else 0
    n_valid = sc_ref[0]

    def dot_qk(hf, g, k):
        return lax.dot_general(qs[hf][g], k, (((1,), (1,)), ((), ())), preferred_element_type=F32)

    worst = jnp.full((1, 1), NEG, F32)
    for hf, g in chains:
        k = kc_ref[:small, :] if use_cache else kn_ref[:small, :]
        m = dot_qk(hf, g, k).max(axis=1, keepdims=True) * scale
        m_ref[rows_of(hf, g), :] = jnp.broadcast_to(m, (bq, 128))
        qf = qs[hf][g].astype(F32)
        size = jnp.sqrt((qf * qf).sum(axis=1, keepdims=True))
        worst = jnp.maximum(worst, (size * (norm_ref[head] * scale) - m).max(axis=0, keepdims=True))
    steady = worst[0, 0] <= 60.0

    def steady_block(live, k, v, mask):
        for hf, g in live:
            rows = rows_of(hf, g)
            s = dot_qk(hf, g, k)
            if mask is not None:
                s = jnp.where(mask, s, NEG)
            m = m_ref[rows, :]
            l = l_ref[rows, :]
            ps = []
            for j in range(k.shape[0] // 128):
                p = jnp.exp2(s[:, j * 128:(j + 1) * 128] * scale - m)
                l = l + p
                ps.append(p.astype(BF16))
            l_ref[rows, :] = l
            acc_ref[rows, :] += jnp.dot(jnp.concatenate(ps, axis=1), v, preferred_element_type=F32)

    def online_block(live, k, v, mask):
        for hf, g in live:
            rows = rows_of(hf, g)
            s = dot_qk(hf, g, k)
            if mask is not None:
                s = jnp.where(mask, s, NEG)
            m_prev = m_ref[rows, :]
            m_new = jnp.maximum(m_prev, s.max(axis=1, keepdims=True) * scale)
            alpha = jnp.exp2(m_prev - m_new)
            p = jnp.exp2(s * scale - m_new[:, :1])
            l_ref[rows, :] = l_ref[rows, :] * alpha + p.sum(axis=1, keepdims=True) * (1.0 / 128)
            m_ref[rows, :] = m_new
            acc_ref[rows, :] = acc_ref[rows, :] * alpha[:, :1] + jnp.dot(p.astype(BF16), v, preferred_element_type=F32)

    def run(block, size):
        joined = use_new and not own and size == 2 * half if use_new else False
        at = lambda i, n: pl.ds(pl.multiple_of(i * n, n), n)
        if use_cache:
            n_full = n_valid // size
            last_block = kc_ref.shape[0] // size - 1

            def step(i, c):
                sl = at(jnp.minimum(i, last_block), size)
                k, v = kc_ref[sl, :], vc_ref[sl, :]
                if joined:
                    k = jnp.where(i >= n_full, kn_ref[...], k)
                    v = jnp.where(i >= n_full, vn_ref[...], v)
                block(chains, k, v, None)
                return c

            lax.fori_loop(0, n_full + (later if joined else 0), step, 0)

            def edge(i, c):
                sl = at(i, small)
                block(chains, kc_ref[sl, :], vc_ref[sl, :], (i * small + lax.broadcasted_iota(jnp.int32, (bq, small), 1)) < n_valid)
                return c

            lax.fori_loop(n_full * (size // small), (n_valid + small - 1) // small, edge, 0)
        if use_new and not own and not (joined and use_cache):
            def new_step(i, c):
                sl = at(i, size)
                block(chains, kn_ref[sl, :], vn_ref[sl, :], None)
                return c

            lax.fori_loop(0, later * (2 * half // size), new_step, 0)
        if own:
            for hf, off in enumerate(offsets):
                live = [(hf, g) for g in range(2)]
                if off:
                    block(live, kn_ref[:off, :], vn_ref[:off, :], None)
                causal = lax.broadcasted_iota(jnp.int32, (bq, bq), 1) <= lax.broadcasted_iota(jnp.int32, (bq, bq), 0)
                block(live, kn_ref[off:off + bq, :], vn_ref[off:off + bq, :], causal)

    @pl.when(steady)
    def _():
        run(steady_block, bk)

    @pl.when(jnp.logical_not(steady))
    def _():
        m_ref[...] = jnp.full_like(m_ref, NEG)
        run(online_block, small)

    lane = lax.broadcasted_iota(jnp.int32, (bq, 128), 1)
    for hf, g in chains:
        c = 2 * hf + g
        rows = slice(c * bq, (c + 1) * bq)
        cs = slice(g * HD, (g + 1) * HD)
        first = 16 * (2 * head + g)
        l = l_ref[rows, :].sum(axis=1, keepdims=True)
        m = jnp.where(l > 0.0, m_ref[rows, 0:1], NEG)
        mine = parts[2 * n_parts * hf:2 * n_parts * (hf + 1)]
        lses = [jnp.where((lane >= first) & (lane < first + 3), a[...].astype(F32), 0.0).sum(axis=1, keepdims=True) for a in mine[1::2]]
        top = functools.reduce(jnp.maximum, lses, m)
        w0 = jnp.exp2(m - top)
        ws = [jnp.exp2(s - top) for s in lses]
        total = functools.reduce(jnp.add, ws, l * w0)
        o = acc_ref[rows, :] * w0
        for p, w in zip(mine[0::2], ws):
            o = o + p[:, cs].astype(F32) * w
        outs[per * hf][:, cs] = (o / total).astype(BF16)
        if want_aux:
            aux_ref = outs[per * hf + 1]
            lse = jnp.broadcast_to(top + jnp.log2(total), (bq, 128))
            aux = aux_ref[...]
            for p, part in enumerate(split3(lse)):
                aux = jnp.where(lane == first + p, part, aux)
            aux_ref[...] = aux


def global_attention(q_list, offsets, own, cache, new, sc, norms, parts, want_aux, bk=1024):
    n_q, bq, _ = q_list[0].shape
    halves = len(q_list)
    n_kv = n_q // 2
    n_parts = len(parts[0])
    kv = lambda a: pl.BlockSpec((a.shape[0], HD), lambda h, *_: (0, h))
    ob = pl.BlockSpec((bq, 2 * HD), lambda h, *_: (0, h))
    ab = pl.BlockSpec((bq, 128), lambda h, *_: (0, 0))
    ins = list(q_list)
    specs = [pl.BlockSpec((2, bq, HD), lambda h, *_: (h, 0, 0))] * halves
    keys = 0
    for group in (cache, new):
        if group is not None:
            ins += list(group)
            specs += [kv(a) for a in group]
            keys += sum(a.shape[0] for a in group) // 2
    for half_parts in parts:
        for o, aux in half_parts:
            ins += [o, aux]
            specs += [ob, ab]
    shapes, out_specs = [], []
    for _ in range(halves):
        shapes.append(jax.ShapeDtypeStruct((bq, n_q * HD), BF16))
        out_specs.append(ob)
        if want_aux:
            shapes.append(jax.ShapeDtypeStruct((bq, 128), BF16))
            out_specs.append(ab)
    m = 2 * halves * bq
    scratch = [pltpu.VMEM((m, 128), F32), pltpu.VMEM((m, 128), F32), pltpu.VMEM((m, HD), F32)]
    if new is not None:
        scratch += [pltpu.VMEM((2 * new[0].shape[0], HD), BF16)] * 2
    rows = halves * bq
    outs = pl.pallas_call(
        functools.partial(global_kernel, tuple(offsets), own, n_parts, bq, bk, cache is not None, new is not None, want_aux),
        grid_spec=pltpu.PrefetchScalarGridSpec(
            num_scalar_prefetch=2, grid=(n_kv,), in_specs=specs, out_specs=out_specs, scratch_shapes=scratch),
        out_shape=shapes, compiler_params=params(1),
        cost_estimate=cost(4 * rows * n_q * keys * HD, 2 * (2 * keys * n_kv * HD + 2 * rows * n_q * HD), rows * n_q * keys),
        name='gattn')(sc, norms, *ins)
    per = 2 if want_aux else 1
    return [tuple(outs[i * per:(i + 1) * per]) for i in range(halves)]


def wo_kernel(at_ref, x_ref, o0_ref, o1_ref, w_ref, near_ref, far_ref, ga_ref, gu_ref, x1_ref, u_ref, all_ref):
    tp, core = at_ref[0], at_ref[1]
    half = w_ref.shape[1]
    piece = near_ref.shape[0]

    @pl.when(pl.program_id(0) == 0)
    def _():
        all_ref[pl.ds(pl.multiple_of(tp * half, half), half), :] = w_ref[0]
        base = (1 - tp) * half
        all_ref[pl.ds(pl.multiple_of(base + core * piece, piece), piece), :] = near_ref[...]
        all_ref[pl.ds(pl.multiple_of(base + (1 - core) * piece, piece), piece), :] = far_ref[...]

    own, other = o0_ref[...], o1_ref[...]
    o = jnp.concatenate([jnp.where(tp == 0, own, other), jnp.where(tp == 0, other, own)], axis=1)
    a = jnp.dot(o, all_ref[...], preferred_element_type=F32).astype(BF16).astype(F32)
    x1 = (x_ref[...].astype(F32) + rms(a, ga_ref[...])).astype(BF16)
    x1_ref[...] = x1
    u_ref[...] = rms(x1.astype(F32), gu_ref[...]).astype(BF16)


def out_proj(layer, at, x, o_own, o_other, w, pieces, ga, gu, row0, tile=256):
    rows, half = o_own.shape
    dim = w.shape[2]
    t0 = row0 // tile
    rowb = pl.BlockSpec((tile, dim), lambda i, *_: (i, 0))
    vec = pl.BlockSpec((1, dim), lambda i, *_: (0, 0))
    ob = pl.BlockSpec((tile, half), lambda i, *_: (i, 0))
    pb = pl.BlockSpec(pieces[0].shape, lambda i, *_: (0, 0))
    return pl.pallas_call(
        wo_kernel,
        grid_spec=pltpu.PrefetchScalarGridSpec(
            num_scalar_prefetch=1, grid=(rows // tile,),
            in_specs=[pl.BlockSpec((tile, dim), lambda i, *_: (i + t0, 0)), ob, ob, pl.BlockSpec((1, half, dim), lambda i, *_: (layer, 0, 0)), pb, pb, vec, vec],
            out_specs=[rowb, rowb], scratch_shapes=[pltpu.VMEM((2 * half, dim), BF16)]),
        out_shape=[jax.ShapeDtypeStruct((rows, dim), BF16)] * 2, compiler_params=params(1),
        cost_estimate=cost(4 * rows * half * dim, 2 * (2 * half * dim + 3 * rows * dim)), name='wo')(at, x, o_own, o_other, w, *pieces, ga, gu)


def ffn_kernel(nb, u_ref, wg_ref, wu_ref, wd_ref, d_ref, act_ref, acc_ref):
    n = pl.program_id(0)

    def head(slot):
        g = jnp.dot(u_ref[...], wg_ref[0], preferred_element_type=F32)
        up = jnp.dot(u_ref[...], wu_ref[0], preferred_element_type=F32)
        act_ref[slot] = (jax.nn.gelu(g, approximate=True) * up).astype(BF16)

    def tail(slot):
        return jnp.dot(act_ref[slot], wd_ref[0], preferred_element_type=F32)

    @pl.when(n == 0)
    def _():
        head(0)
        acc_ref[...] = jnp.zeros_like(acc_ref)

    for slot in range(2):
        @pl.when((n > 0) & (n < nb) & (n % 2 == slot))
        def _():
            acc_ref[...] += tail(1 - slot)
            head(slot)

    @pl.when(n == nb)
    def _():
        d_ref[...] = (acc_ref[...] + tail((nb - 1) % 2)).astype(BF16)


def ffn(layer, u, wg, wu, wd, bn=512):
    rows, dim = u.shape
    width = wg.shape[2]
    nb = width // bn
    return pl.pallas_call(
        functools.partial(ffn_kernel, nb), grid=(nb + 1,),
        in_specs=[pl.BlockSpec((rows, dim), lambda n: (0, 0)),
                  pl.BlockSpec((1, dim, bn), lambda n: (layer, 0, jnp.minimum(n, nb - 1))),
                  pl.BlockSpec((1, dim, bn), lambda n: (layer, 0, jnp.minimum(n, nb - 1))),
                  pl.BlockSpec((1, bn, dim), lambda n: (layer, jnp.maximum(n - 1, 0), 0))],
        out_specs=pl.BlockSpec((rows, dim), lambda n: (0, 0)),
        out_shape=jax.ShapeDtypeStruct((rows, dim), BF16),
        scratch_shapes=[pltpu.VMEM((2, rows, bn), BF16), pltpu.VMEM((rows, dim), F32)],
        compiler_params=params(1),
        cost_estimate=cost(6 * rows * dim * width, 2 * (3 * dim * width + 2 * rows * dim), rows * width), name='ffn')(u, wg, wu, wd)


def last_kernel(x_ref, d0_ref, d1_ref, g_ref, *rest):
    d = (d0_ref[...].astype(F32) + d1_ref[...].astype(F32)).astype(BF16).astype(F32)
    rest[-1][...] = (x_ref[...].astype(F32) + rms(d, g_ref[...])).astype(BF16)


def last(x, d_pair, gain, total_rows, row0, carried, tile=256):
    rows, dim = x.shape
    t0 = row0 // tile
    rowb = pl.BlockSpec((tile, dim), lambda i: (i, 0))
    ins = [x, d_pair[0], d_pair[1], gain]
    specs = [rowb, rowb, rowb, pl.BlockSpec((1, dim), lambda i: (0, 0))]
    aliases = {}
    if carried is not None:
        aliases[4] = 0
        ins.append(carried)
        specs.append(pl.BlockSpec(memory_space=pl.ANY))
    return pl.pallas_call(
        last_kernel, grid=(rows // tile,), in_specs=specs,
        out_specs=pl.BlockSpec((tile, dim), lambda i: (i + t0, 0)),
        out_shape=jax.ShapeDtypeStruct((total_rows, dim), BF16), input_output_aliases=aliases,
        compiler_params=params(1), cost_estimate=cost(10 * rows * dim, 8 * rows * dim), name='last')(*ins)


def rope_tables(positions, base, divisor):
    inv_freq = 1.0 / (base ** (jnp.arange(0, HD, 2, dtype=F32) / HD))
    angles = (positions.astype(F32) / divisor)[:, None] * inv_freq[None, :]
    return jnp.cos(angles), jnp.sin(angles)


def solution(mesh):
    cp_size = mesh.shape['cp']
    tp_size = mesh.shape['tp']
    row_spec = P(('dp', 'cp'), None)
    cache_spec = P(('dp', 'cp'), 'tp', None)
    window_spec = P('dp', 'tp', None)
    col_spec = P(None, None, 'tp')
    row_split = P(None, 'tp', None)
    replicated = P()

    def device_step(hidden, start_pos, k_local, v_local, k_global, v_global, w_query, w_key, w_value, w_out, w_gate, w_up, w_down, norm_gain, qk_gain):
        first_pos = start_pos[0]
        cp_index = lax.axis_index('cp')
        tp_index = lax.axis_index('tp')
        core = jnp.remainder(cp_index, 2)
        at = jnp.stack([tp_index, core]).astype(jnp.int32)
        rows = hidden.shape[0]
        part = rows // 2
        n_kv = k_local.shape[1]
        shard_len = k_global.shape[0]
        positions = first_pos + cp_index * rows + jnp.arange(rows)
        gains = lambda l, i: norm_gain[l, i][None, :]
        move = lambda a, k: lax.ppermute(a, 'cp', [(i, i ^ k) for i in range(cp_size)])
        swap = lambda a: lax.ppermute(a, 'tp', [(i, tp_size - 1 - i) for i in range(tp_size)])
        after = lambda a, dep: lax.optimization_barrier((a, dep))[0]

        def out_weights(l, src):
            n = src.shape[1] // 2
            return swap(lax.dynamic_slice(src, (l, core * n, 0), (1, n, src.shape[2]))[0])

        def both_pieces(mine, dep):
            mine = after(mine, dep)
            return mine, move(mine, 1)

        def finish(l, i, x, row0, o, pieces):
            x1, u = out_proj(l, at, x, o, swap(o), w_out, pieces, gains(l, 1), gains(l, 2), row0)
            d = ffn(l, u, w_gate, w_up, w_down)
            return x1, (d, swap(d))

        piece = out_weights(0, w_out)
        cos, sin = rope_tables(positions, 10000.0, 1.0)
        k0, k1, v0, v1, h = kv_first(0, hidden, gains(0, 0), qk_gain[0], w_key, w_value, cos, sin)
        ahead = [(i, i + 1) for i in range(cp_size - 1)]
        pass_on = lambda a: lax.ppermute(a, 'cp', ahead)
        got = {1: (pass_on(k1), pass_on(v1)), 0: (pass_on(k0), pass_on(v0))}
        got[1], got[0] = lax.optimization_barrier((got[1], got[0]))
        shift = jnp.remainder(first_pos, k_local.shape[0])
        rolled = [jnp.roll(c.reshape(c.shape[0], -1), -shift, axis=0) for c in (k_local, v_local)]
        q = q_after(0, h, qk_gain[0], w_query, cos, sin)
        flag = cp_index.astype(jnp.int32)[None]
        xs, ds, os = {}, {}, {}
        own = (k0, k1, v0, v1)
        os[1] = window_attention(flag, q, got, rolled, own, (1,), part, part)
        os[0] = window_attention(after(flag, os[1]), q, got, rolled, own, (0, 1), 0, part)
        pieces = both_pieces(piece, os[0])
        for i in (1, 0):
            xs[i], ds[i] = finish(0, i, hidden, i * part, os[i], pieces)

        cos, sin = rope_tables(positions, 1000000.0, 8.0)
        q, k_new, v_new, mids = {}, {}, {}, {}
        def project(i, x):
            q[i], k_new[i], v_new[i], mids[i] = qkv(1, x, ds[i], gains(0, 3), gains(1, 0), qk_gain[1], w_query, w_key, w_value, cos, sin, i * part)

        project(1, xs[1])
        cache = [c.reshape(shard_len, -1) for c in (k_global, v_global)]
        n_valid = jnp.clip(first_pos - cp_index * shard_len, 0, shard_len)
        new = []
        widest = lambda a, live: jnp.sqrt(jnp.where(live[:, None], jnp.sum(jnp.square(a.astype(F32)), axis=-1), 0.0).max(axis=0))
        norms = {False: widest(k_global, jnp.arange(shard_len) < n_valid)}

        def attend(qh, owner, halves, parts, want_aux, use_cache=True, use_new=True):
            sc = jnp.stack([n_valid, (owner - cp_index) * rows]).astype(jnp.int32)
            return global_attention([qh[i] for i in halves], [i * part for i in halves], owner is cp_index, cache if use_cache else None, new if use_new else None, sc, norms[use_new], parts, want_aux)

        send = lambda pair, k: tuple(move(a, k) for a in pair)
        q1, q2, q3 = {}, {}, {}

        def spread(i):
            q1[i], q2[i] = move(q[i], 1), move(q[i], 2)

        spread(1)
        q3[1] = move(q2[1], 1)
        o1, o2, o3, own = {}, {}, {}, {}
        early, = attend(q1, cp_index ^ 1, (1,), [[]], True, use_new=False)
        project(0, after(xs[0], (early[0], q2[1])))
        new += [k_new[0], k_new[1], v_new[0], v_new[1]]
        norms[True] = functools.reduce(jnp.maximum, [widest(k_new[i].reshape(part, n_kv, HD), jnp.full((part,), True)) for i in (0, 1)], norms[False])
        spread(0)
        o1[0], = attend(q1, cp_index ^ 1, (0,), [[]], True)
        q2[0] = after(q2[0], o1[0][0])
        q3[0] = move(q2[0], 1)
        o2[0], o2[1] = attend(q2, cp_index ^ 2, (0, 1), [[], []], True)
        got2 = {i: send(o2[i], 1) for i in (0, 1)}
        q1[1] = after(q1[1], o2[0][0])
        o1[1], = attend(q1, cp_index ^ 1, (1,), [[early]], True, use_cache=False)
        q3[0] = after(q3[0], o1[1][0])
        o3[0], = attend(q3, cp_index ^ 3, (0,), [[got2[0]]], True)
        q3[1] = after(q3[1], o3[0][0])
        o3[1], = attend(q3, cp_index ^ 3, (1,), [[got2[1]]], True)
        pieces = both_pieces(out_weights(1, after(w_out, o1[0][0])), o3[0][0])
        got1 = {i: send(o1[i], 1) for i in (0, 1)}
        got3 = {i: send(o3[i], 3) for i in (0, 1)}
        q[0] = after(q[0], o3[1][0])
        (own[0],), = attend(q, cp_index, (0,), [[got1[0], got3[0]]], False)
        q[1] = after(q[1], own[0])
        (own[1],), = attend(q, cp_index, (1,), [[got1[1], got3[1]]], False)
        out = None
        for i in (0, 1):
            xs[i], ds[i] = finish(1, i, mids[i], 0, own[i], pieces)
        for i in (0, 1):
            out = last(xs[i], ds[i], gains(1, 3), rows, i * part, out)
        heads = lambda a: a.reshape(rows, n_kv, HD)
        join = lambda a, b: heads(jnp.concatenate([a, b], axis=0))
        return out, join(k0, k1), join(v0, v1), join(k_new[0], k_new[1]), join(v_new[0], v_new[1])

    return jax.shard_map(device_step, mesh=mesh, in_specs=(row_spec, P('dp'), window_spec, window_spec, cache_spec, cache_spec, col_spec, col_spec, col_spec, row_split, col_spec, col_spec, row_split, replicated, replicated), out_specs=(row_spec, cache_spec, cache_spec, cache_spec, cache_spec), check_vma=False)
```
